128 devices in a mesh: rep: 2 (over core), dp: 64 (over x, y, z).
Axes of the slice: x: 4, y: 4, z: 4, core: 2. Of those that a mesh axis runs over, the one named last changes fastest.
Arguments:
- x: bfloat16 [128, 2048, 896], P(('rep', 'dp')), parts along dimension 0
- dy: bfloat16 [128, 2048, 896], P(('rep', 'dp')), parts along dimension 0
- w_gate: bfloat16 [2, 896, 4864], P(None, 'dp')
- w_up: bfloat16 [2, 896, 4864], P(None, 'dp')
- w_down: bfloat16 [2, 4864, 896], P(None, 'dp')
- m_w_gate: float32 [2, 896, 4864], P(None, 'dp')
- m_w_up: float32 [2, 896, 4864], P(None, 'dp')
- m_w_down: float32 [2, 4864, 896], P(None, 'dp')
- v_w_gate: float32 [2, 896, 4864], P(None, 'dp')
- v_w_up: float32 [2, 896, 4864], P(None, 'dp')
- v_w_down: float32 [2, 4864, 896], P(None, 'dp')
Outputs:
- output 1: bfloat16 [4, 896, 4864], P('rep', 'dp'), parts along dimension 0
- output 2: bfloat16 [4, 896, 4864], P('rep', 'dp'), parts along dimension 0
- output 3: bfloat16 [4, 4864, 896], P('rep', 'dp'), parts along dimension 0
- output 4: float32 [4, 896, 4864], P('rep', 'dp'), parts along dimension 0
- output 5: float32 [4, 896, 4864], P('rep', 'dp'), parts along dimension 0
- output 6: float32 [4, 4864, 896], P('rep', 'dp'), parts along dimension 0
- output 7: float32 [4, 896, 4864], P('rep', 'dp'), parts along dimension 0
- output 8: float32 [4, 896, 4864], P('rep', 'dp'), parts along dimension 0
- output 9: float32 [4, 4864, 896], P('rep', 'dp'), parts along dimension 0
There are 2 independent parts. The reference program is written for one: setup_inputs(seed, part) draws one part's arguments, and reference() takes and returns one part's arrays. A program takes and returns all parts, laid end to end along the dimension named above; an argument that names none is the same for every part.
All inputs are finite; a program needn't handle non-finite values.
Results may differ from the reference program's by a relative error of at most 0.0235.
Values are sent between devices in bfloat16 or wider.
A program may use at most 1.5 GiB of HBM per device.

```python
import jax
import jax.numpy as jnp
from jax import lax

SEQUENCES = 64
TOKENS = 2048
D = 896
FF = 4864
LAYERS = 2
NAMES = ("w_gate", "w_up", "w_down")
SHAPES = {"w_gate": (LAYERS, D, FF), "w_up": (LAYERS, D, FF), "w_down": (LAYERS, FF, D)}


def bump(key, n, height):
    away = (jnp.arange(n, dtype=jnp.int32) - jax.random.randint(key, (), 0, n, jnp.int32)) % n
    return jnp.where(away < n // 8, height, 1.0)


def together(key, own, strength):
    shared = jax.random.normal(key, own.shape[1:], jnp.float32)
    return (own + strength * shared) * lax.rsqrt(1 + strength * strength)


def setup_inputs(seed: int = 0, part: int = 0) -> dict:
    kx, kdy, ka, kb, kz, kf, kh, kl, *keys = jax.random.split(jax.random.key(seed), 8 + 3 * len(NAMES))
    kx, kdy, ka, kb = (jax.random.fold_in(k, part) for k in (kx, kdy, ka, kb))
    kw, km, kv = (keys[i::3] for i in range(3))
    shape = (SEQUENCES, TOKENS, D)
    much_x, much_dy = jax.random.uniform(kz, (2,), jnp.float32, 0.0, 1.0)
    loud = 2.0 ** jax.random.uniform(jax.random.fold_in(kz, 1), (), jnp.float32, -1.0, 2.0)
    layers = 2.0 ** jax.random.uniform(kl, (LAYERS, 1, 1), jnp.float32, -1.0, 1.0)
    x = together(ka, jax.random.normal(kx, shape, jnp.float32), much_x) * bump(kf, D, 4.0)
    dy = together(kb, jax.random.normal(kdy, shape, jnp.float32), much_dy)
    drawn = {"x": x.astype(jnp.bfloat16), "dy": (loud * dy * (SEQUENCES * TOKENS) ** -0.5).astype(jnp.bfloat16)}
    for key, name in zip(kw, NAMES, strict=True):
        w = jax.random.normal(key, SHAPES[name], jnp.float32) * SHAPES[name][1] ** -0.5
        drawn[name] = (w * {"w_gate": 1.0, "w_up": bump(kh, FF, 4.0), "w_down": layers}[name]).astype(jnp.bfloat16)
    for key, name in zip(km, NAMES, strict=True):
        drawn[f"m_{name}"] = 0.1 * jax.random.normal(key, SHAPES[name], jnp.float32)
    for key, name in zip(kv, NAMES, strict=True):
        drawn[f"v_{name}"] = loud * loud * jax.random.uniform(key, SHAPES[name], jnp.float32, 0.05, 0.15)
    return drawn


def matmul(a, w):
    return jnp.dot(a, w, preferred_element_type=jnp.float32).astype(jnp.bfloat16)


def normed(h):
    wide = h.astype(jnp.float32)
    scale = lax.rsqrt(jnp.mean(wide**2, -1, keepdims=True) + 1e-6)
    return (wide * scale).astype(jnp.bfloat16)


def layer(h, w):
    a = normed(h)
    gate = jnp.dot(a, w["w_gate"], preferred_element_type=jnp.float32)
    up = jnp.dot(a, w["w_up"], preferred_element_type=jnp.float32)
    return h + matmul((jax.nn.silu(gate) * up).astype(jnp.bfloat16), w["w_down"])


def adamw(w, m, v, g):
    m = 0.9 * m + 0.1 * g
    v = 0.95 * v + 0.05 * g * g
    step = m * lax.rsqrt(v + 1e-8) + 0.1 * w
    return (w - 0.02 * step).astype(jnp.bfloat16), m, v


def stack(weights, h):
    return lax.scan(lambda h, w: (layer(h, w), None), h, weights)[0]


def reference(x, dy, w_gate, w_up, w_down, m_w_gate, m_w_up, m_w_down, v_w_gate, v_w_up, v_w_down):
    weights = dict(zip(NAMES, (w_gate, w_up, w_down), strict=True))

    def take(so_far, sequence):
        h, by_y = sequence
        _, back = jax.vjp(lambda w: stack(w, h), weights)
        return jax.tree.map(lambda total, term: total + term.astype(jnp.float32), so_far, back(by_y)[0]), None

    none_yet = {name: jnp.zeros(w.shape, jnp.float32) for name, w in weights.items()}
    by_weights, _ = lax.scan(take, none_yet, (x, dy))
    gradients = [by_weights[name].astype(jnp.bfloat16).astype(jnp.float32) for name in NAMES]
    new = [
        adamw(w.astype(jnp.float32), m, v, g)
        for w, m, v, g in zip((w_gate, w_up, w_down), (m_w_gate, m_w_up, m_w_down), (v_w_gate, v_w_up, v_w_down), gradients, strict=True)
    ]
    return tuple(one[which] for which in range(3) for one in new)
```

```python
import jax
import jax.numpy as jnp
from jax import lax
from jax.sharding import PartitionSpec as P


BF, F32 = jnp.bfloat16, jnp.float32
X, Y, Z = 4, 4, 4
PLANE = [[(x * Y + y) * Z + z for x in range(X) for y in range(Y)] for z in range(Z)]


def dot(a, b, contract):
    return lax.dot_general(a, b, ((contract[:1], contract[1:]), ((), ())), preferred_element_type=F32)


def normed(h):
    wide = h.astype(F32)
    scale = lax.rsqrt(jnp.mean(wide**2, -1, keepdims=True) + 1e-6)
    return (wide * scale).astype(BF)


def adamw(w, m, v, g):
    m = 0.9 * m + 0.1 * g
    v = 0.95 * v + 0.05 * g * g
    step = m * lax.rsqrt(v + 1e-8) + 0.1 * w
    return (w - 0.02 * step).astype(BF), m, v


def shifted(a, by):
    pairs = [(p * Z + (z + by) % Z, p * Z + z) for p in range(X * Y) for z in range(Z)]
    return lax.ppermute(a, "dp", pairs)


def scattered(pairs, rows):
    terms = [dot(a, b, (0, 0)).astype(BF) for a, b in pairs]
    columns = terms[0].shape[1]
    part = lax.psum_scatter(jnp.concatenate(terms, 1), "dp", scatter_dimension=0, axis_index_groups=PLANE, tiled=True)
    z = lax.axis_index("dp") % Z
    blocks = part.reshape(Z, rows, part.shape[1])
    total = lax.dynamic_index_in_dim(blocks, z, 0, keepdims=False).astype(F32)
    for by in range(1, Z):
        theirs = lax.dynamic_index_in_dim(blocks, (z + Z - by) % Z, 0, keepdims=False)
        total += shifted(theirs, by).astype(F32)
    return [total[:, i * columns : (i + 1) * columns] for i in range(len(terms))]


def solution(mesh):
    n = mesh.shape["dp"]

    def step(x, dy, *arrays):
        weights, ms, vs = (arrays[i : i + 3] for i in (0, 3, 6))
        layers, rows, ff = weights[0].shape
        d = n * rows
        deep = weights[2].shape[1]
        tall, high = 16, 80
        i = lax.broadcasted_iota(jnp.int32, (d, n * tall), 0)
        j = lax.broadcasted_iota(jnp.int32, (d, n * tall), 1)
        place = (j == i // rows * tall + i % rows).astype(BF)

        first = lax.axis_index("rep") == 0

        def sided(one, two):
            return jnp.where(first, one, two), jnp.where(first, two, one)

        def gathered_in(number):
            mine = jnp.pad(sided(weights[0][number], weights[1][number])[0], ((0, tall - rows), (0, 0)))[None]
            mine = lax.all_gather(mine, "dp", axis=0, tiled=True).reshape(n * tall, ff)
            return mine, lax.ppermute(mine, "rep", [(0, 1), (1, 0)])

        def gathered_out(number):
            one = jnp.pad(weights[2][number], ((0, high - deep), (0, 0)))[None]
            return lax.all_gather(one, "dp", axis=0, tiled=True)[:, :deep].reshape(ff, d)

        w_in, w_out = [], []
        for number in range(layers):
            w_in.append(gathered_in(number))
            w_out.append(gathered_out(number))

        h, saved = x[0], []
        for number in range(layers):
            a = normed(h)
            wide = dot(a, place, (1, 0)).astype(BF)
            mine = dot(wide, w_in[number][0], (1, 0))
            other = dot(wide, w_in[number][1], (1, 0))
            gate, up = sided(mine, other)
            product = (gate * jax.nn.sigmoid(gate) * up).astype(BF)
            saved.append((h, a, mine, other, product))
            if number < layers - 1:
                out = dot(product, w_out[number], (1, 0)).astype(BF)
                h = h + out

        by_h, g = dy[0], [None] * layers
        for number in reversed(range(layers)):
            h, a, mine, other, product = saved[number]
            gate, up = sided(mine, other)
            by_h, product = lax.optimization_barrier((by_h, product))
            g_down = scattered([(product, by_h)], deep)[0]
            by_product = dot(by_h, w_out[number], (1, 1)).astype(BF).astype(F32)
            sig = jax.nn.sigmoid(gate)
            by_in = sided(up * (sig * (1 + gate * (1 - sig))), gate * sig)
            by_in = lax.optimization_barrier(tuple((by_product * factor).astype(BF) for factor in by_in))
            g[number] = (*sided(*scattered([(a, by) for by in by_in], rows)), g_down)
            if number > 0:
                by_mine, by_other = (dot(by, w, (1, 1)).astype(BF) for by, w in zip(by_in, w_in[number], strict=True))
                by_a = dot(by_mine + by_other, place, (1, 1)).astype(BF)
                by_h = by_h + jax.vjp(normed, h)[1](by_a)[0]

        new = []
        for which in range(3):
            one = jnp.stack([g[number][which] for number in range(layers)], 1).astype(BF).astype(F32)
            w, m, v = (jnp.swapaxes(given[which], 0, 1) for given in (weights, ms, vs))
            new.append([jnp.swapaxes(got, 0, 1) for got in adamw(w.astype(F32), m, v, one)])
        return tuple(one[which] for which in range(3) for one in new)

    states, cut = P(("rep", "dp"), None, None), P(None, "dp", None)
    return jax.shard_map(
        step,
        mesh=mesh,
        in_specs=(states, states) + (cut,) * 9,
        out_specs=(P("rep", "dp", None),) * 9,
        check_vma=False,
    )
```
